32 devices in a mesh: lon: 4 (over y, x), lat: 8 (over z, core).
Axes of the slice: x: 2, y: 2, z: 4, core: 2. Of those that a mesh axis runs over, the one named last changes fastest.
Arguments:
- meridional_speed: float32 [16, 512, 1024], P(None, 'lat', 'lon'), may hold values from -6 to 6
- theta_field: float32 [16, 512, 1024], P(None, 'lat', 'lon'), may hold values from -2 to 30
- tier_vertical_span: float32 [16], replicated, may hold values from 0.5 to 4
- grid_zonal_span: float32 [512, 1024], P('lat', 'lon'), may hold values from 0.05 to 40
- grid_plan_extent: float32 [512, 1024], P('lat', 'lon'), may hold values from 0.2 to 5
- ocean_energy_input: float32 [512, 1024], P('lat', 'lon'), may hold values from -6 to 6
- ocean_tier_tally: int32 [512, 1024], P('lat', 'lon'), may hold values from 0 to 16, as said below
- grid_region_label: int32 [512, 1024], P('lat', 'lon'), may hold values from 0 to 3
- seam_matching_meridian: int32 [1024], P('lon'), may hold values from 0 to 1023, as said below
Outputs:
- class_transport: float32 [4, 512, 128], P(None, 'lat')
- overturning: float32 [4, 512, 16], P(None, 'lat')
- heat_transport: float32 [4, 512], P(None, 'lat')
- implied_transport: float32 [4, 512], P(None, 'lat')
The draws below stay inside these ranges and needn't reach their ends.
Inputs may be any that keep to these rules, and one draw needn't show every extreme that they name: `ocean_tier_tally`: one column, the same at every latitude, has at least one wet level, and every column of the northernmost row has at least one. seam_matching_meridian[i] = (c - i) mod 1024 for a c that each draw picks.
All inputs are finite; a program needn't handle non-finite values.
Results may differ from the reference program's by a relative error of at most 0.0003.
Values sent between devices are 32-bit elements; how exact they have to be, the bound alone decides.
A program may use at most 64 MiB of HBM per device.

```python
import math
import jax
import jax.numpy as jnp
from jax import lax

LOCAL_PARALLELS = 64
VERTICAL_TIERS = 16
THERMAL_BINS = 128
OCEAN_REGIONS = 4
GRID_MERIDIANS = 1024
GRID_PARALLELS = 512


def draw_grid_zonal_span(key, part):
    column = jnp.arange(GRID_MERIDIANS, dtype=jnp.float32)[None, :] / (GRID_MERIDIANS - 1.0)
    base_width = jnp.exp(jax.random.uniform(key, (GRID_PARALLELS, GRID_MERIDIANS), jnp.float32, jnp.log(0.3), jnp.log(3.0)))
    return (base_width * jnp.exp(jnp.log(3.0) * column)).astype(jnp.float32)


def draw_ocean_tier_tally(key, part):
    raw_depth = jax.random.randint(key, (GRID_PARALLELS, GRID_MERIDIANS), -(VERTICAL_TIERS // 3), VERTICAL_TIERS + 1, dtype=jnp.int32)
    col_depth = jnp.maximum(raw_depth, 0)
    wet_column = jax.random.randint(jax.random.fold_in(key, 11), (), 0, GRID_MERIDIANS, dtype=jnp.int32)
    column_ids = jnp.arange(GRID_MERIDIANS, dtype=jnp.int32)[None, :]
    row_ids = jnp.arange(GRID_PARALLELS, dtype=jnp.int32)[:, None]
    forced = (column_ids == wet_column) | (row_ids == GRID_PARALLELS - 1)
    return jnp.where(forced, jnp.maximum(col_depth, 1), col_depth).astype(jnp.int32)


def draw_seam_matching_meridian(key, part):
    centre = jax.random.randint(key, (), 0, GRID_MERIDIANS, dtype=jnp.int32)
    column_ids = jnp.arange(GRID_MERIDIANS, dtype=jnp.int32)
    return jnp.mod(centre - column_ids + GRID_MERIDIANS, GRID_MERIDIANS).astype(jnp.int32)


def place_ends(array, rng, least, largest):
    shape = array.shape
    spot = [jax.random.randint(jax.random.fold_in(rng, axis), (), 0, shape[axis]) for axis in range(len(shape))]
    array = array.at[tuple(spot)].set(least)
    longest = shape.index(max(shape))
    spot[longest] = (spot[longest] + 1) % shape[longest]
    return array.at[tuple(spot)].set(largest)


def level_of(own_key, dims, shards, low, largest):
    factor_of, own = 1.0, jax.random.fold_in(own_key, 6)
    for position, blocks in shards:
        draws = jnp.exp(jax.random.uniform(jax.random.fold_in(own, position), (blocks,), jnp.float32, low / len(shards), largest / len(shards)))
        factor_of = factor_of * jnp.repeat(draws, dims[position] // blocks).reshape([-1 if axis == position else 1 for axis in range(len(dims))])
    return factor_of


def gaussian(rng, shape, scale, bound, split=(), held_as=jnp.bfloat16):
    array = jax.random.normal(rng, shape, jnp.float32) * scale
    if len(split) > 0:
        array = level_of(rng, shape, split, -0.22, 0.18) * array
    return jnp.clip(array, min=-bound, max=bound).astype(held_as)


def setup_inputs(seed: int = 0) -> dict:
    splits = jax.random.split(jax.random.key(seed), 10)
    meridional_speed = gaussian(splits[0], (VERTICAL_TIERS, GRID_PARALLELS, GRID_MERIDIANS), 1.0, 6.0, ((1, 8), (2, 4)), jnp.float32)
    theta_field = jnp.clip(-2.0 + 32.0 * jax.random.uniform(splits[1], (VERTICAL_TIERS, GRID_PARALLELS, GRID_MERIDIANS), jnp.float32) ** level_of(splits[1], (VERTICAL_TIERS, GRID_PARALLELS, GRID_MERIDIANS), ((1, 8), (2, 4)), -0.2, 0.2), -2.0, 30.0)
    tier_vertical_span = jnp.clip(jnp.exp(jax.random.uniform(splits[2], (VERTICAL_TIERS,), jnp.float32, math.log(0.5), math.log(4.0))), 0.5, 4.0)
    grid_zonal_span = draw_grid_zonal_span(jax.random.fold_in(splits[9], 71), 0)
    grid_plan_extent = jnp.clip(jnp.exp(math.log(5.0) - 3.218876 * jax.random.uniform(splits[4], (GRID_PARALLELS, GRID_MERIDIANS), jnp.float32) ** level_of(splits[4], (GRID_PARALLELS, GRID_MERIDIANS), ((0, 8), (1, 4)), -0.2, 0.2)), 0.2, 5.0)
    ocean_energy_input = gaussian(splits[5], (GRID_PARALLELS, GRID_MERIDIANS), 1.0, 6.0, ((0, 8), (1, 4)), jnp.float32)
    ocean_tier_tally = draw_ocean_tier_tally(jax.random.fold_in(splits[9], 71), 0)
    grid_region_label = place_ends(jax.random.randint(splits[7], (GRID_PARALLELS, GRID_MERIDIANS), 0, OCEAN_REGIONS), jax.random.fold_in(splits[7], 1), 0, OCEAN_REGIONS - 1).astype(jnp.int32)
    seam_matching_meridian = draw_seam_matching_meridian(jax.random.fold_in(splits[9], 71), 0)
    return {"meridional_speed": meridional_speed, "theta_field": theta_field, "tier_vertical_span": tier_vertical_span, "grid_zonal_span": grid_zonal_span, "grid_plan_extent": grid_plan_extent, "ocean_energy_input": ocean_energy_input, "ocean_tier_tally": ocean_tier_tally, "grid_region_label": grid_region_label, "seam_matching_meridian": seam_matching_meridian}


THERMAL_FLOOR = -2.0
THERMAL_RANGE = 32.0

def vertical_aggregate_field(meridional_speed, theta_field, tier_vertical_span, grid_zonal_span, grid_plan_extent, ocean_energy_input, ocean_tier_tally, grid_region_label, subsequent_theta, subsequent_vertical_extent, theta_bucket_tally, region_tally):
    tier_ordinal, parallel_tally, meridian_tally = theta_field.shape
    poleward_theta = jnp.concatenate([theta_field[:, 1:, :], subsequent_theta[:, None, :]], axis=1)
    interface_theta = 0.5 * (theta_field + poleward_theta)
    north_depth = jnp.concatenate([ocean_tier_tally[1:, :], subsequent_vertical_extent[None, :]], axis=0)
    face_depth = jnp.minimum(ocean_tier_tally, north_depth)
    level_iota = lax.broadcasted_iota(jnp.int32, (tier_ordinal, 1, 1), 0)
    wet_mask = (level_iota < face_depth[None, :, :]).astype(jnp.float32)
    water_capacity = wet_mask * tier_vertical_span[:, None, None] * grid_zonal_span[None, :, :]
    mass_conveyance = water_capacity * meridional_speed
    bucket_spacing = THERMAL_RANGE / theta_bucket_tally
    placement_offset = jnp.clip((interface_theta - THERMAL_FLOOR) / bucket_spacing, 0.0, theta_bucket_tally - 1.0)
    lower_real_value = jnp.minimum(jnp.floor(placement_offset), theta_bucket_tally - 2.0)
    upper_interp_factor = placement_offset - lower_real_value
    parallel_ramp = lax.broadcasted_iota(jnp.int32, (1, parallel_tally, 1), 1)
    group_labels = (grid_region_label[None, :, :] * parallel_tally + parallel_ramp) * theta_bucket_tally + lower_real_value.astype(jnp.int32)
    group_labels = group_labels.reshape(-1)
    bucket_aggregate = jax.ops.segment_sum(jnp.concatenate([(mass_conveyance * (1.0 - upper_interp_factor)).reshape(-1), (mass_conveyance * upper_interp_factor).reshape(-1)]), jnp.concatenate([group_labels, group_labels + 1]), num_segments=region_tally * parallel_tally * theta_bucket_tally)
    bucket_aggregate = bucket_aggregate.reshape(region_tally, parallel_tally, theta_bucket_tally)
    basin_iota = lax.broadcasted_iota(jnp.int32, (region_tally, 1, 1), 0)
    bucket_membership = (grid_region_label[None, :, :] == basin_iota).astype(jnp.float32)
    level_sum = jnp.einsum('bji,kji->bjk', bucket_membership, mass_conveyance, precision=lax.Precision.HIGHEST)
    energy_aggregate = jnp.einsum('dwk,wk->dw', bucket_membership, lax.optimization_barrier(jnp.sum(mass_conveyance * interface_theta, axis=0)), precision=lax.Precision.HIGHEST)
    parallel_theta_field = lax.optimization_barrier(jnp.sum(water_capacity * interface_theta, axis=(0, 2)))
    row_wet = lax.optimization_barrier(jnp.sum(water_capacity, axis=(0, 2)))
    flux_rows = jnp.einsum('dwk,wk->dw', bucket_membership, ocean_energy_input * grid_plan_extent, precision=lax.Precision.HIGHEST)
    return (bucket_aggregate, level_sum, energy_aggregate, parallel_theta_field, row_wet, flux_rows)

def finish_rows(bucket_aggregate, level_sum, energy_aggregate, parallel_theta_field, row_wet, unit_scale):
    row_mean = parallel_theta_field / row_wet
    volume_total = lax.optimization_barrier(jnp.sum(level_sum, axis=2))
    heat_out = unit_scale / 16.0 * (energy_aggregate - volume_total * row_mean[None, :])
    stream = unit_scale * jnp.cumsum(level_sum, axis=2)
    return (unit_scale * bucket_aggregate, stream, heat_out)

def reference(meridional_speed, theta_field, tier_vertical_span, grid_zonal_span, grid_plan_extent, ocean_energy_input, ocean_tier_tally, grid_region_label, seam_matching_meridian):
    reflected_theta = jnp.take(theta_field[:, GRID_PARALLELS - 1, :], seam_matching_meridian, axis=1)
    mirror_depth = jnp.take(ocean_tier_tally[GRID_PARALLELS - 1, :], seam_matching_meridian, axis=0)
    unit_scale = math.sqrt(THERMAL_BINS / (GRID_MERIDIANS * VERTICAL_TIERS))

    def row_block(parallel_initial_offset):
        tile_theta_field = lax.dynamic_slice_in_dim(theta_field, parallel_initial_offset, LOCAL_PARALLELS, 1)
        tile_speed_field = lax.dynamic_slice_in_dim(meridional_speed, parallel_initial_offset, LOCAL_PARALLELS, 1)
        tile_vertical_extent = lax.dynamic_slice_in_dim(ocean_tier_tally, parallel_initial_offset, LOCAL_PARALLELS, 0)
        tile_zonal_span = lax.dynamic_slice_in_dim(grid_zonal_span, parallel_initial_offset, LOCAL_PARALLELS, 0)
        tile_plan_extent = lax.dynamic_slice_in_dim(grid_plan_extent, parallel_initial_offset, LOCAL_PARALLELS, 0)
        tile_energy_input = lax.dynamic_slice_in_dim(ocean_energy_input, parallel_initial_offset, LOCAL_PARALLELS, 0)
        tile_region_label = lax.dynamic_slice_in_dim(grid_region_label, parallel_initial_offset, LOCAL_PARALLELS, 0)
        subsequent_offset = jnp.minimum(parallel_initial_offset + LOCAL_PARALLELS, GRID_PARALLELS - 1).astype(jnp.int32)
        final_flag = parallel_initial_offset + LOCAL_PARALLELS >= GRID_PARALLELS
        next_theta_value = lax.dynamic_slice_in_dim(theta_field, subsequent_offset, 1, 1)[:, 0, :]
        later_vertical_extent = lax.dynamic_slice_in_dim(ocean_tier_tally, subsequent_offset, 1, 0)[0]
        next_theta_value = jnp.where(final_flag, reflected_theta, next_theta_value)
        later_vertical_extent = jnp.where(final_flag, mirror_depth, later_vertical_extent)
        return vertical_aggregate_field(tile_speed_field, tile_theta_field, tier_vertical_span, tile_zonal_span, tile_plan_extent, tile_energy_input, tile_vertical_extent, tile_region_label, next_theta_value, later_vertical_extent, THERMAL_BINS, OCEAN_REGIONS)
    starts = jnp.arange(GRID_PARALLELS // LOCAL_PARALLELS, dtype=jnp.int32) * LOCAL_PARALLELS
    bucket_aggregate, level_sum, energy_aggregate, parallel_theta_field, row_wet, flux_rows = lax.map(row_block, starts)
    bucket_aggregate = jnp.transpose(bucket_aggregate, (1, 0, 2, 3)).reshape(OCEAN_REGIONS, GRID_PARALLELS, THERMAL_BINS)
    level_sum = jnp.transpose(level_sum, (1, 0, 2, 3)).reshape(OCEAN_REGIONS, GRID_PARALLELS, VERTICAL_TIERS)
    energy_aggregate = jnp.transpose(energy_aggregate, (1, 0, 2)).reshape(OCEAN_REGIONS, GRID_PARALLELS)
    flux_rows = jnp.transpose(flux_rows, (1, 0, 2)).reshape(OCEAN_REGIONS, GRID_PARALLELS)
    parallel_theta_field = parallel_theta_field.reshape(GRID_PARALLELS)
    row_wet = row_wet.reshape(GRID_PARALLELS)
    class_out, stream, heat_out = finish_rows(bucket_aggregate, level_sum, energy_aggregate, parallel_theta_field, row_wet, unit_scale)
    implied = 2.0 / math.sqrt(GRID_MERIDIANS * GRID_PARALLELS) * jnp.cumsum(flux_rows, axis=1)
    return (class_out, stream, heat_out, implied)
```

```python
import functools
import math

import jax
import jax.numpy as jnp
from jax import lax
from jax.experimental import pallas as pl
from jax.experimental.pallas import tpu as pltpu
from jax.sharding import PartitionSpec as P

THERMAL_BINS = 128
OCEAN_REGIONS = 4
THERMAL_FLOOR = -2.0
THERMAL_RANGE = 32.0

ROWS = 8
DIGIT = 15
HIGHS = -(-(THERMAL_BINS - 1) // DIGIT)
GROUP = 4
STRIDE = 32
MESH = pl.DeviceIdType.MESH
NT = (((1,), (1,)), ((), ()))
HIGHEST = lax.Precision.HIGHEST
BF = jnp.bfloat16
F32 = jnp.float32


def iota(shape, dim):
    return lax.broadcasted_iota(jnp.int32, shape, dim)


def two_parts(x):
    high = x.astype(BF).astype(F32)
    return jnp.concatenate([high, x - high], axis=0).astype(BF)


def exact_parts(x):
    high = x.astype(BF).astype(F32)
    rest = x - high
    mid = rest.astype(BF).astype(F32)
    return jnp.concatenate([high.astype(BF), mid.astype(BF), (rest - mid).astype(BF)], axis=0)


def kernel(
    nlon, nlat, width_total, height_total,
    dz, speed_h, theta_h, dx_h, area_h, flux_h, depth_h, region_h, seam,
    raw,
    speed_v, theta_v, dx_v, area_v, flux_v, depth_v, region_v,
    edge, edge_in, top, top_in, fx, fx_in, total, total_in, buf, got,
    big_sem, small_sem, edge_sem, top_send, top_recv, fx_send, fx_recv, tot_send, tot_recv,
    sum_send, sum_recv,
):
    tiers, blocks, _, width = theta_h.shape
    height = blocks * ROWS
    mylon, mylat = lax.axis_index("lon"), lax.axis_index("lat")
    implied_scale = 2.0 / math.sqrt(width_total * height_total)
    last = blocks - 1

    barrier = pltpu.get_barrier_semaphore()
    for step in range(1, nlon):
        peer = lax.rem(mylon + step, nlon)
        pl.semaphore_signal(barrier, inc=1, device_id=(peer, mylat), device_id_type=MESH)
    for step in range(1, nlat):
        peer = lax.rem(mylat + step, nlat)
        pl.semaphore_signal(barrier, inc=1, device_id=(mylon, peer), device_id_type=MESH)

    small = [
        pltpu.make_async_copy(src, dst, small_sem.at[n])
        for n, (src, dst) in enumerate(
            [
                (area_h, area_v),
                (flux_h, flux_v),
                (region_h, region_v),
                (depth_h, depth_v.at[pl.ds(0, blocks)]),
                (dx_h, dx_v),
            ]
        )
    ]

    def theta_copy(b):
        return pltpu.make_async_copy(theta_h.at[:, b], theta_v.at[b], big_sem.at[0, b])

    def speed_copy(b):
        return pltpu.make_async_copy(speed_h.at[:, b], speed_v.at[b], big_sem.at[1, b])

    for copy in small:
        copy.start()
    theta_copy(0).start()
    theta_copy(last).start()
    for b in range(blocks):
        speed_copy(b).start()
        if b + 1 < last:
            theta_copy(b + 1).start()
    for copy in small:
        copy.wait()

    region_all = region_v[...].reshape(height, width)
    product = flux_v[...].reshape(height, width) * area_v[...].reshape(height, width)
    fx_rows = jnp.zeros((ROWS, height), F32)
    for b in range(OCEAN_REGIONS):
        part = lax.dot_general(
            jnp.ones((ROWS, width), F32),
            jnp.where(region_all == b, product, 0.0),
            NT, precision=HIGHEST, preferred_element_type=F32,
        )
        fx_rows = jnp.where(iota((ROWS, height), 0) == b, part, fx_rows)
    fx[...] = jnp.zeros_like(fx)
    fx[:, pl.ds(0, height)] = fx_rows

    theta_copy(0).wait()
    theta_copy(last).wait()
    edge[...] = jnp.zeros_like(edge)
    top[...] = jnp.zeros_like(top)
    for k in range(tiers):
        edge[pl.ds(k, 1), :] = theta_v[0, k, pl.ds(0, 1), :]
        top[pl.ds(k, 1), :] = theta_v[last, k, pl.ds(ROWS - 1, 1), :]
    edge[pl.ds(tiers, 1), :] = depth_v[0, pl.ds(0, 1), :].astype(F32)
    top[pl.ds(tiers, 1), :] = depth_v[last, pl.ds(ROWS - 1, 1), :].astype(F32)

    pl.semaphore_wait(barrier, nlon - 1 + nlat - 1)

    edge_copy = pltpu.make_async_remote_copy(
        edge, edge_in, edge_sem.at[0], edge_sem.at[1],
        device_id=(mylon, lax.rem(mylat + nlat - 1, nlat)), device_id_type=MESH,
    )

    def to_lon(src, dst, send, recv, step):
        return pltpu.make_async_remote_copy(
            src, dst.at[step - 1], send.at[step - 1], recv.at[step - 1],
            device_id=(lax.rem(mylon + step, nlon), mylat), device_id_type=MESH,
        )

    def to_lat(step):
        return pltpu.make_async_remote_copy(
            total, total_in.at[step - 1], tot_send.at[step - 1], tot_recv.at[step - 1],
            device_id=(mylon, lax.rem(mylat + step, nlat)), device_id_type=MESH,
        )

    edge_copy.start()
    for step in range(1, nlon):
        to_lon(fx, fx_in, fx_send, fx_recv, step).start()

    @pl.when(mylat == nlat - 1)
    def _():
        for step in range(1, nlon):
            to_lon(top, top_in, top_send, top_recv, step).start()

    def across(offset):
        peer = mylon
        for bit in range(nlon.bit_length() - 1):
            stride = 1 << bit
            if offset & stride:
                peer = peer + stride * (1 - 2 * lax.rem(lax.div(mylon, stride), 2))
        return peer

    def share(offset, src, dst):
        return pltpu.make_async_remote_copy(
            src, dst, sum_send.at[offset - 1], sum_recv.at[offset - 1],
            device_id=(across(offset), mylat), device_id_type=MESH,
        )

    def tree(parts):
        while len(parts) > 1:
            parts = [parts[n] + parts[n + 1] for n in range(0, len(parts), 2)]
        return parts[0]

    def compute(jb):
        reg = region_v[jb].astype(F32)
        dx = dx_v[jb]
        deep = depth_v[jb]
        wet = jnp.minimum(
            deep, jnp.concatenate([deep[1:], depth_v[jb + 1][:1]], axis=0)
        )
        one, zero = jnp.ones((2 * ROWS, width), BF), jnp.zeros((2 * ROWS, width), BF)
        heat = jnp.zeros((ROWS, width), F32)
        warm = jnp.zeros((ROWS, width), F32)
        water = jnp.zeros((ROWS, width), F32)
        levels = []
        acc = None
        for first in range(0, tiers, GROUP):
            lefts, rights = [], []
            for k in range(first, min(first + GROUP, tiers)):
                th = theta_v[jb, k]
                north = jnp.concatenate([th[1:], theta_v[jb + 1, k][:1]], axis=0)
                face = 0.5 * (th + north)
                volume = jnp.where(k < wet, dz[k] * dx, 0.0)
                moved = volume * speed_v[jb, k]
                heat = heat + moved * face
                warm = warm + volume * face
                water = water + volume
                place = jnp.clip(
                    (face - THERMAL_FLOOR) * (THERMAL_BINS / THERMAL_RANGE),
                    0.0, THERMAL_BINS - 1.0,
                )
                low = jnp.minimum(jnp.floor(place), THERMAL_BINS - 2.0)
                upper = moved * (place - low)
                under = moved - upper
                high = jnp.floor((low + 0.5) * (1.0 / DIGIT))
                digit = low - DIGIT * high
                pick = high * OCEAN_REGIONS + reg
                pick2 = jnp.concatenate([pick, pick - 1.0], axis=0).astype(BF)
                digit2 = jnp.concatenate([digit, digit], axis=0).astype(BF)
                under2, upper2 = two_parts(under), two_parts(upper)
                levels.append(two_parts(moved))
                lefts.append(
                    jnp.concatenate(
                        [
                            jnp.where(pick2 == jnp.asarray(2 * n, BF), one, zero)
                            for n in range(HIGHS * OCEAN_REGIONS // 2)
                        ],
                        axis=0,
                    )
                )
                hits = [digit2 == jnp.asarray(n, BF) for n in range(DIGIT)]
                tent = [jnp.where(hits[0], under2, zero)]
                for n in range(1, DIGIT):
                    tent.append(jnp.where(hits[n], under2, jnp.where(hits[n - 1], upper2, zero)))
                tent.append(jnp.where(hits[DIGIT - 1], upper2, zero))
                rights.append(jnp.concatenate(tent, axis=0))
            part = lax.dot_general(
                jnp.concatenate(lefts, axis=1), jnp.concatenate(rights, axis=1), NT,
                preferred_element_type=F32,
            )
            acc = part if acc is None else acc + part

        def collapse(full):
            rows, cols = full.shape
            same = (iota((ROWS, cols), 0) == iota((ROWS, cols), 1) % ROWS)
            full = jnp.where(
                same[None], full.reshape(rows // ROWS, ROWS, cols), 0.0
            ).reshape(rows, cols)
            spread = (iota((cols, 128), 0) // (2 * ROWS) == iota((cols, 128), 1))
            out = jnp.dot(
                two_parts(full), jnp.where(spread, 1.0, 0.0).astype(BF),
                preferred_element_type=F32,
            )
            return out[:rows] + out[rows:]

        sums = collapse(acc)
        for b in range(OCEAN_REGIONS):
            line = sums[b * ROWS : (b + 1) * ROWS]
            for h in range(1, HIGHS):
                at = (h * OCEAN_REGIONS + b) * ROWS
                line = line + pltpu.roll(sums[at : at + ROWS], h * DIGIT, 1)
            buf[jb, pl.ds(b * ROWS, ROWS), :] = line
        reg2 = jnp.concatenate([reg, reg - 1.0], axis=0).astype(BF)
        basin = jnp.concatenate(
            [
                jnp.where(reg2 == jnp.asarray(2 * n, BF), one, zero)
                for n in range(OCEAN_REGIONS // 2)
            ],
            axis=0,
        )
        kept = levels + [two_parts(heat), two_parts(warm), two_parts(water)]
        while len(kept) % 8:
            kept.append(zero)
        table = collapse(
            lax.dot_general(
                basin, jnp.concatenate(kept, axis=0), NT, preferred_element_type=F32
            )
        )
        line = table[:ROWS]
        for b in range(1, OCEAN_REGIONS):
            line = line + pltpu.roll(table[b * ROWS : (b + 1) * ROWS], b * STRIDE, 1)
        buf[jb, pl.ds(OCEAN_REGIONS * ROWS, ROWS), :] = line

    def northern_row():
        @pl.when(mylat < nlat - 1)
        def _():
            for k in range(tiers):
                theta_v[blocks, k, pl.ds(0, 1), :] = edge_in[pl.ds(k, 1), :]
            depth_v[blocks, pl.ds(0, 1), :] = edge_in[pl.ds(tiers, 1), :].astype(jnp.int32)

        @pl.when(mylat == nlat - 1)
        def _():
            found = jnp.zeros((3 * top.shape[0], width), F32)
            for step in range(nlon):
                if step:
                    to_lon(top, top_in, top_send, top_recv, step).wait()
                block = top_in[step - 1] if step else top[...]
                owner = lax.rem(mylon + nlon - step, nlon)
                here = iota((width, width), 0) + owner * width == seam[...]
                found = found + jnp.dot(
                    exact_parts(block), jnp.where(here, 1.0, 0.0).astype(BF),
                    preferred_element_type=F32,
                )
            n = top.shape[0]
            row = found[:n] + found[n : 2 * n] + found[2 * n :]
            top[...] = row
            for k in range(tiers):
                theta_v[blocks, k, pl.ds(0, 1), :] = top[pl.ds(k, 1), :]
            depth_v[blocks, pl.ds(0, 1), :] = top[pl.ds(tiers, 1), :].astype(jnp.int32)

    def flux_middle():
        for step in range(1, nlon):
            to_lon(fx, fx_in, fx_send, fx_recv, step).wait()
        mine = fx[...]
        whole = jnp.zeros_like(mine)
        for owner in range(nlon):
            piece = mine
            for step in range(1, nlon):
                came = lax.rem(mylon + nlon - step, nlon)
                piece = jnp.where(came == owner, fx_in[step - 1], piece)
            whole = whole + piece
        fx[...] = whole
        total[...] = jnp.broadcast_to(jnp.sum(whole, axis=1, keepdims=True), total.shape)
        for step in range(1, nlat):
            to_lat(step).start()

    def flux_end():
        for step in range(1, nlat):
            to_lat(step).wait()
        before = jnp.zeros(total.shape, F32)
        for step in range(1, nlat):
            before = before + jnp.where(mylat >= step, total_in[step - 1], 0.0)
        until = (iota((height, height), 0) <= iota((height, height), 1)).astype(F32)
        run = jnp.dot(
            fx[:, pl.ds(0, height)], until, precision=HIGHEST, preferred_element_type=F32
        )
        out = implied_scale * (before[:, :1] + run)
        raw[blocks, 0, :, pl.ds(0, height)] = out

    def iteration(it, carry):
        speed_copy(it).wait()

        @pl.when(it + 1 < last)
        def _():
            theta_copy(it + 1).wait()

        @pl.when(it == min(3, last))
        def _():
            flux_middle()

        @pl.when(it == last)
        def _():
            edge_copy.wait()
            northern_row()

        compute(it)
        for offset in range(1, nlon):
            share(offset, buf.at[it], got.at[offset - 1, it]).start()
        return carry

    lax.fori_loop(0, blocks, iteration, 0)
    flux_end()
    for offset in range(1, nlon):
        share(offset, buf, got.at[offset - 1]).wait()
    for jb in range(blocks):
        both = tree([buf[jb]] + [got[offset - 1, jb] for offset in range(1, nlon)])
        raw[jb] = both.reshape(OCEAN_REGIONS + 1, ROWS, 128)


def finish(width_total, raw, class_o, stream_o, heat_o, implied_o):
    blocks, height = raw.shape[0] - 1, stream_o.shape[2]
    tiers = stream_o.shape[1]
    unit_scale = math.sqrt(THERMAL_BINS / (width_total * tiers))
    for b in range(OCEAN_REGIONS):
        class_o[b] = unit_scale * raw[:blocks, b]
    implied_o[...] = raw[blocks, 0, :OCEAN_REGIONS, :height]
    table = raw[:blocks, OCEAN_REGIONS].reshape(height, 128)
    dst, src = iota((128, 128), 0), iota((128, 128), 1)
    chain = (src // STRIDE == dst // STRIDE) & (src <= dst) & (src % STRIDE < tiers)
    stream = unit_scale * lax.dot_general(
        chain.astype(F32), table, NT, precision=HIGHEST, preferred_element_type=F32
    )
    for b in range(OCEAN_REGIONS):
        stream_o[b] = stream[b * STRIDE : b * STRIDE + tiers]
    row, lane = iota((4 * ROWS, 128), 0), iota((4 * ROWS, 128), 1)
    kind, place, slot = row // ROWS, row % ROWS, lane % STRIDE
    own = place == lane // STRIDE
    choose = (
        ((kind == 0) & own & (slot == tiers))
        | ((kind == 1) & own & (slot < tiers))
        | ((kind == 2) & (slot == tiers + 1))
        | ((kind == 3) & (slot == tiers + 2))
    )
    rows = lax.dot_general(
        choose.astype(F32), table, NT, precision=HIGHEST, preferred_element_type=F32
    )
    mean = rows[2 * ROWS : 3 * ROWS] / rows[3 * ROWS :]
    heat = (unit_scale / 16.0) * (rows[:ROWS] - rows[ROWS : 2 * ROWS] * mean)
    heat_o[...] = heat[:OCEAN_REGIONS]


def body(speed, theta, dz, dx, area, flux, depth, region, seam):
    tiers, height, width = theta.shape
    nlon, nlat = lax.axis_size("lon"), lax.axis_size("lat")
    blocks = height // ROWS
    edge_rows = -(-(tiers + 1) // 8) * 8
    pad = -(-height // 128) * 128
    flat = (blocks, ROWS, width)
    any_spec = pl.BlockSpec(memory_space=pltpu.HBM)
    vmem = pl.BlockSpec(memory_space=pltpu.VMEM)
    dma = pltpu.SemaphoreType.DMA
    raw = pl.pallas_call(
        functools.partial(kernel, nlon, nlat, width * nlon, height * nlat),
        name="transport",
        out_shape=jax.ShapeDtypeStruct((blocks + 1, OCEAN_REGIONS + 1, ROWS, pad), F32),
        in_specs=[pl.BlockSpec(memory_space=pltpu.SMEM)] + [any_spec] * 7 + [vmem],
        out_specs=vmem,
        scratch_shapes=[
            pltpu.VMEM((blocks, tiers, ROWS, width), F32),
            pltpu.VMEM((blocks + 1, tiers, ROWS, width), F32),
            pltpu.VMEM(flat, F32),
            pltpu.VMEM(flat, F32),
            pltpu.VMEM(flat, F32),
            pltpu.VMEM((blocks + 1, ROWS, width), jnp.int32),
            pltpu.VMEM(flat, jnp.int32),
            pltpu.VMEM((edge_rows, width), F32),
            pltpu.VMEM((edge_rows, width), F32),
            pltpu.VMEM((edge_rows, width), F32),
            pltpu.VMEM((nlon - 1, edge_rows, width), F32),
            pltpu.VMEM((ROWS, pad), F32),
            pltpu.VMEM((nlon - 1, ROWS, pad), F32),
            pltpu.VMEM((ROWS, 128), F32),
            pltpu.VMEM((nlat - 1, ROWS, 128), F32),
            pltpu.VMEM((blocks, 5 * ROWS, 128), F32),
            pltpu.VMEM((nlon - 1, blocks, 5 * ROWS, 128), F32),
            dma((2, blocks)),
            dma((5,)),
            dma((2,)),
            dma((nlon - 1,)),
            dma((nlon - 1,)),
            dma((nlon - 1,)),
            dma((nlon - 1,)),
            dma((nlat - 1,)),
            dma((nlat - 1,)),
            dma((nlon - 1,)),
            dma((nlon - 1,)),
        ],
        compiler_params=pltpu.CompilerParams(
            collective_id=0, has_side_effects=True, vmem_limit_bytes=67043328 - (blocks + 1) * (OCEAN_REGIONS + 1) * ROWS * pad * 4 - 8192
        ),
    )(
        dz,
        speed.reshape(tiers, *flat),
        theta.reshape(tiers, *flat),
        dx.reshape(flat),
        area.reshape(flat),
        flux.reshape(flat),
        depth.reshape(flat),
        region.reshape(flat),
        seam.reshape(1, width),
    )
    out = pl.pallas_call(
        functools.partial(finish, width * nlon),
        name="finish",
        out_shape=(
            jax.ShapeDtypeStruct((OCEAN_REGIONS, blocks, ROWS, THERMAL_BINS), F32),
            jax.ShapeDtypeStruct((OCEAN_REGIONS, tiers, height), F32),
            jax.ShapeDtypeStruct((OCEAN_REGIONS, height), F32),
            jax.ShapeDtypeStruct((OCEAN_REGIONS, height), F32),
        ),
        in_specs=[vmem],
        out_specs=(vmem,) * 4,
        compiler_params=pltpu.CompilerParams(vmem_limit_bytes=8 << 20),
    )(raw)
    classes = out[0].reshape(OCEAN_REGIONS, height, THERMAL_BINS)
    return (classes, jnp.swapaxes(out[1], 1, 2), out[2], out[3])


def solution(mesh):
    in_specs = (
        P(None, "lat", "lon"),
        P(None, "lat", "lon"),
        P(),
        P("lat", "lon"),
        P("lat", "lon"),
        P("lat", "lon"),
        P("lat", "lon"),
        P("lat", "lon"),
        P("lon"),
    )
    out_specs = (P(None, "lat", None), P(None, "lat", None), P(None, "lat"), P(None, "lat"))
    return jax.shard_map(body, mesh=mesh, in_specs=in_specs, out_specs=out_specs, check_vma=False)
```

```python
import functools
import math

import jax
import jax.numpy as jnp
from jax import lax
from jax.experimental import pallas as pl
from jax.experimental.pallas import tpu as pltpu
from jax.sharding import PartitionSpec as P

THERMAL_BINS = 128
OCEAN_REGIONS = 4
THERMAL_FLOOR = -2.0
THERMAL_RANGE = 32.0

ROWS = 8
DIGIT = 16
HIGHS = THERMAL_BINS // DIGIT
PAIRS = OCEAN_REGIONS // 2
GROUP = 4
STRIDE = 32
MESH = pl.DeviceIdType.MESH
NT = (((1,), (1,)), ((), ()))
HIGHEST = lax.Precision.HIGHEST
BF = jnp.bfloat16
F32 = jnp.float32


def iota(shape, dim):
    return lax.broadcasted_iota(jnp.int32, shape, dim)


def two_parts(x):
    high = x.astype(BF).astype(F32)
    return jnp.concatenate([high, x - high], axis=0).astype(BF)


def exact_parts(x):
    high = x.astype(BF).astype(F32)
    rest = x - high
    mid = rest.astype(BF).astype(F32)
    return jnp.concatenate([high.astype(BF), mid.astype(BF), (rest - mid).astype(BF)], axis=0)


def kernel(
    nlon, nlat, width_total, height_total,
    dz, speed, theta, dx_all, area, flux, depth, region, seam,
    raw,
    edge, edge_in, top, top_in, cap, fx, fx_in, total, total_in, buf, got,
    edge_sem, top_send, top_recv, fx_send, fx_recv, tot_send, tot_recv,
    sum_send, sum_recv,
):
    tiers, blocks, _, width = theta.shape
    height = blocks * ROWS
    mylon, mylat = lax.axis_index("lon"), lax.axis_index("lat")
    implied_scale = 2.0 / math.sqrt(width_total * height_total)
    last = blocks - 1

    barrier = pltpu.get_barrier_semaphore()
    for step in range(1, nlon):
        peer = lax.rem(mylon + step, nlon)
        pl.semaphore_signal(barrier, inc=1, device_id=(peer, mylat), device_id_type=MESH)
    for step in range(1, nlat):
        peer = lax.rem(mylat + step, nlat)
        pl.semaphore_signal(barrier, inc=1, device_id=(mylon, peer), device_id_type=MESH)

    def flux_start():
        region_all = region[...].reshape(height, width)
        product = flux[...].reshape(height, width) * area[...].reshape(height, width)
        fx_rows = jnp.zeros((ROWS, height), F32)
        for b in range(OCEAN_REGIONS):
            part = lax.dot_general(
                jnp.ones((ROWS, width), F32),
                jnp.where(region_all == b, product, 0.0),
                NT, precision=HIGHEST, preferred_element_type=F32,
            )
            fx_rows = jnp.where(iota((ROWS, height), 0) == b, part, fx_rows)
        fx[...] = jnp.zeros_like(fx)
        fx[:, pl.ds(0, height)] = fx_rows

    edge[...] = jnp.zeros_like(edge)
    top[...] = jnp.zeros_like(top)
    for k in range(tiers):
        edge[pl.ds(k, 1), :] = theta[k, 0, pl.ds(0, 1), :]
        top[pl.ds(k, 1), :] = theta[k, last, pl.ds(ROWS - 1, 1), :]
    edge[pl.ds(tiers, 1), :] = depth[0, pl.ds(0, 1), :].astype(F32)
    top[pl.ds(tiers, 1), :] = depth[last, pl.ds(ROWS - 1, 1), :].astype(F32)
    flux_start()

    edge_copy = pltpu.make_async_remote_copy(
        edge, edge_in, edge_sem.at[0], edge_sem.at[1],
        device_id=(mylon, lax.rem(mylat + nlat - 1, nlat)), device_id_type=MESH,
    )

    def to_lon(src, dst, send, recv, step):
        return pltpu.make_async_remote_copy(
            src, dst.at[step - 1], send.at[step - 1], recv.at[step - 1],
            device_id=(lax.rem(mylon + step, nlon), mylat), device_id_type=MESH,
        )

    def to_lat(step):
        return pltpu.make_async_remote_copy(
            total, total_in.at[step - 1], tot_send.at[step - 1], tot_recv.at[step - 1],
            device_id=(mylon, lax.rem(mylat + step, nlat)), device_id_type=MESH,
        )

    def across(offset):
        peer = mylon
        for bit in range(nlon.bit_length() - 1):
            stride = 1 << bit
            if offset & stride:
                peer = peer + stride * (1 - 2 * lax.rem(lax.div(mylon, stride), 2))
        return peer

    def share(offset, src, dst):
        return pltpu.make_async_remote_copy(
            src, dst, sum_send.at[offset - 1], sum_recv.at[offset - 1],
            device_id=(across(offset), mylat), device_id_type=MESH,
        )

    def tree(parts):
        while len(parts) > 1:
            parts = [parts[n] + parts[n + 1] for n in range(0, len(parts), 2)]
        return parts[0]

    def first_sends():
        pl.semaphore_wait(barrier, nlon - 1 + nlat - 1)
        edge_copy.start()
        for step in range(1, nlon):
            to_lon(fx, fx_in, fx_send, fx_recv, step).start()

        @pl.when(mylat == nlat - 1)
        def _():
            for step in range(1, nlon):
                to_lon(top, top_in, top_send, top_recv, step).start()

    def compute(jb, cap_row):
        reg = region[jb].astype(F32)
        dx = dx_all[jb]
        deep = depth[jb].astype(F32)

        def above(own, k):
            row = theta[k, jb + 1, pl.ds(0, 1), :] if cap_row is None else cap_row(k)
            return jnp.concatenate([own[1:], row], axis=0)

        def twice(x, y):
            return jnp.concatenate([x, y], axis=0).astype(BF)

        depth_row = (
            depth[jb + 1, pl.ds(0, 1), :].astype(F32) if cap_row is None else cap_row(tiers)
        )
        wet = jnp.minimum(deep, jnp.concatenate([deep[1:], depth_row], axis=0))
        one, zero = jnp.ones((2 * ROWS, width), BF), jnp.zeros((2 * ROWS, width), BF)
        reg2 = twice(reg, reg - 1.0)
        here = [
            jnp.where(reg2 == jnp.asarray(2 * n, BF), one, zero) for n in range(PAIRS)
        ]
        heat = jnp.zeros((ROWS, width), F32)
        warm = jnp.zeros((ROWS, width), F32)
        water = jnp.zeros((ROWS, width), F32)
        kept = []
        acc = None
        for first in range(0, tiers, GROUP):
            tents, picks = [], []
            for k in range(first, min(first + GROUP, tiers)):
                th = theta[k, jb]
                both = th + above(th, k)
                face = 0.5 * both
                volume = jnp.where(wet > float(k), dz[k] * dx, 0.0)
                moved = volume * speed[k, jb]
                heat = heat + moved * face
                warm = warm + volume * face
                water = water + volume
                place = jnp.clip(
                    (face - THERMAL_FLOOR) * (THERMAL_BINS / THERMAL_RANGE),
                    0.0, THERMAL_BINS - 1.0,
                )
                low = jnp.minimum(jnp.floor(place), THERMAL_BINS - 2.0)
                upper = moved * (place - low)
                under = moved - upper
                high = jnp.floor(low * (1.0 / DIGIT))
                digit = low - DIGIT * high
                high2 = twice(high, high)
                digit2 = twice(digit, digit - 8.0)
                under_h = under.astype(BF).astype(F32)
                upper_h = upper.astype(BF).astype(F32)
                under_l, upper_l = under - under_h, upper - upper_h
                hits = [digit2 == jnp.asarray(n, BF) for n in range(-1, 8)]
                tent = []
                for low_half, high_half in ((under_h, upper_h), (under_l, upper_l)):
                    low2, up2 = twice(low_half, low_half), twice(high_half, high_half)
                    for n in range(8):
                        tent.append(
                            jnp.where(hits[n + 1], low2, jnp.where(hits[n], up2, zero))
                        )
                ending = twice(digit, digit) == jnp.asarray(DIGIT - 1, BF)
                tent.append(jnp.where(ending, twice(upper_h, upper_l), zero))
                tents.append(jnp.concatenate(tent, axis=0))
                kept.append(two_parts(moved))
                chosen = [high2 == jnp.asarray(n, BF) for n in range(HIGHS)]
                picks.append(
                    jnp.concatenate(
                        [
                            jnp.where(chosen[n], here[pair], zero)
                            for pair in range(PAIRS)
                            for n in range(HIGHS)
                        ],
                        axis=0,
                    )
                )
            part = lax.dot_general(
                jnp.concatenate(tents, axis=1), jnp.concatenate(picks, axis=1), NT,
                preferred_element_type=F32,
            )
            acc = part if acc is None else acc + part

        lane = iota((ROWS, 128), 1)
        row = iota((ROWS, 128), 0)

        def align(x, slot):
            source = (lane + row + (128 - slot)) % 128
            return jnp.take_along_axis(x, source, axis=1, mode="promise_in_bounds")

        for pair in range(PAIRS):
            cols = acc[:, 128 * pair : 128 * pair + 128]
            held = []
            for half in range(2):
                out = jnp.zeros((ROWS, 128), F32)
                for n in range(8):
                    at = 16 * n + 8 * half
                    one_tent = cols[at : at + ROWS] + cols[128 + at : 128 + at + ROWS]
                    out = jnp.where(lane % 8 == n, align(one_tent, n), out)
                held.append(out)
            final = cols[256 : 256 + ROWS] + cols[256 + ROWS :]
            held[0] = held[0] + jnp.where(lane % 8 == 0, align(final, DIGIT), 0.0)
            left = lane % 16 < 8
            buf[jb, pl.ds(2 * pair * ROWS, ROWS), :] = jnp.where(
                left, held[0], pltpu.roll(held[1], 8, 1)
            )
            buf[jb, pl.ds((2 * pair + 1) * ROWS, ROWS), :] = jnp.where(
                left, pltpu.roll(held[0], 120, 1), held[1]
            )
        kept = kept + [two_parts(heat), two_parts(warm), two_parts(water)]
        nothing = jnp.zeros((ROWS, width), F32)
        basin = []
        for b in range(OCEAN_REGIONS):
            basin += [twice(jnp.where(reg == float(b), 1.0, 0.0), nothing), zero]
        table = lax.dot_general(
            jnp.concatenate(kept, axis=0), jnp.concatenate(basin, axis=0), NT,
            preferred_element_type=F32,
        )
        line = jnp.zeros((ROWS, 128), F32)
        for k in range(len(kept)):
            at = 2 * ROWS * k
            whole = table[at : at + ROWS] + table[at + ROWS : at + 2 * ROWS]
            line = jnp.where(lane % STRIDE == k, align(whole, k), line)
        buf[jb, pl.ds(OCEAN_REGIONS * ROWS, ROWS), :] = line
        for offset in range(1, nlon):
            share(offset, buf.at[jb], got.at[offset - 1, jb]).start()

    def northern_row():
        edge_copy.wait()

        @pl.when(mylat < nlat - 1)
        def _():
            cap[...] = edge_in[...]

        @pl.when(mylat == nlat - 1)
        def _():
            found = jnp.zeros((3 * top.shape[0], width), F32)
            for step in range(nlon):
                if step:
                    to_lon(top, top_in, top_send, top_recv, step).wait()
                block = top_in[step - 1] if step else top[...]
                owner = lax.rem(mylon + nlon - step, nlon)
                here = iota((width, width), 0) + owner * width == seam[...]
                found = found + jnp.dot(
                    exact_parts(block), jnp.where(here, 1.0, 0.0).astype(BF),
                    preferred_element_type=F32,
                )
            n = top.shape[0]
            cap[...] = found[:n] + found[n : 2 * n] + found[2 * n :]

    def flux_middle():
        for step in range(1, nlon):
            to_lon(fx, fx_in, fx_send, fx_recv, step).wait()
        mine = fx[...]
        whole = jnp.zeros_like(mine)
        for owner in range(nlon):
            piece = mine
            for step in range(1, nlon):
                came = lax.rem(mylon + nlon - step, nlon)
                piece = jnp.where(came == owner, fx_in[step - 1], piece)
            whole = whole + piece
        fx[...] = whole
        total[...] = jnp.broadcast_to(jnp.sum(whole, axis=1, keepdims=True), total.shape)
        for step in range(1, nlat):
            to_lat(step).start()

    def flux_end():
        for step in range(1, nlat):
            to_lat(step).wait()
        before = jnp.zeros(total.shape, F32)
        for step in range(1, nlat):
            before = before + jnp.where(mylat >= step, total_in[step - 1], 0.0)
        until = (iota((height, height), 0) <= iota((height, height), 1)).astype(F32)
        run = jnp.dot(
            fx[:, pl.ds(0, height)], until, precision=HIGHEST, preferred_element_type=F32
        )
        out = implied_scale * (before[:, :1] + run)
        raw[blocks, 0, :, pl.ds(0, height)] = out

    def iteration(it, carry):
        @pl.when(it == min(4, last - 1))
        def _():
            flux_middle()

        compute(it, None)
        return carry

    first_sends()
    lax.fori_loop(0, last, iteration, 0)
    northern_row()
    compute(last, lambda k: cap[pl.ds(k, 1), :])
    flux_end()
    for offset in range(1, nlon):
        share(offset, buf, got.at[offset - 1]).wait()
    for jb in range(blocks):
        both = tree([buf[jb]] + [got[offset - 1, jb] for offset in range(1, nlon)])
        raw[jb] = both.reshape(OCEAN_REGIONS + 1, ROWS, 128)


def finish(width_total, raw, class_o, stream_o, heat_o, implied_o):
    blocks, height = raw.shape[0] - 1, stream_o.shape[2]
    tiers = stream_o.shape[1]
    unit_scale = math.sqrt(THERMAL_BINS / (width_total * tiers))
    for b in range(OCEAN_REGIONS):
        class_o[b] = unit_scale * raw[:blocks, b]
    implied_o[...] = raw[blocks, 0, :OCEAN_REGIONS, :height]
    table = raw[:blocks, OCEAN_REGIONS].reshape(height, 128)
    dst, src = iota((128, 128), 0), iota((128, 128), 1)
    chain = (src // STRIDE == dst // STRIDE) & (src <= dst) & (src % STRIDE < tiers)
    stream = unit_scale * lax.dot_general(
        chain.astype(F32), table, NT, precision=HIGHEST, preferred_element_type=F32
    )
    for b in range(OCEAN_REGIONS):
        stream_o[b] = stream[b * STRIDE : b * STRIDE + tiers]
    row, lane = iota((4 * ROWS, 128), 0), iota((4 * ROWS, 128), 1)
    kind, place, slot = row // ROWS, row % ROWS, lane % STRIDE
    own = place == lane // STRIDE
    choose = (
        ((kind == 0) & own & (slot == tiers))
        | ((kind == 1) & own & (slot < tiers))
        | ((kind == 2) & (slot == tiers + 1))
        | ((kind == 3) & (slot == tiers + 2))
    )
    rows = lax.dot_general(
        choose.astype(F32), table, NT, precision=HIGHEST, preferred_element_type=F32
    )
    mean = rows[2 * ROWS : 3 * ROWS] / rows[3 * ROWS :]
    heat = (unit_scale / 16.0) * (rows[:ROWS] - rows[ROWS : 2 * ROWS] * mean)
    heat_o[...] = heat[:OCEAN_REGIONS]


def body(speed, theta, dz, dx, area, flux, depth, region, seam):
    tiers, height, width = theta.shape
    nlon, nlat = lax.axis_size("lon"), lax.axis_size("lat")
    blocks = height // ROWS
    edge_rows = -(-(tiers + 1) // 8) * 8
    pad = -(-height // 128) * 128
    flat = (blocks, ROWS, width)
    vmem = pl.BlockSpec(memory_space=pltpu.VMEM)
    dma = pltpu.SemaphoreType.DMA
    raw = pl.pallas_call(
        functools.partial(kernel, nlon, nlat, width * nlon, height * nlat),
        name="transport",
        out_shape=jax.ShapeDtypeStruct((blocks + 1, OCEAN_REGIONS + 1, ROWS, pad), F32),
        in_specs=[pl.BlockSpec(memory_space=pltpu.SMEM)] + [vmem] * 8,
        out_specs=vmem,
        scratch_shapes=[
            pltpu.VMEM((edge_rows, width), F32),
            pltpu.VMEM((edge_rows, width), F32),
            pltpu.VMEM((edge_rows, width), F32),
            pltpu.VMEM((nlon - 1, edge_rows, width), F32),
            pltpu.VMEM((edge_rows, width), F32),
            pltpu.VMEM((ROWS, pad), F32),
            pltpu.VMEM((nlon - 1, ROWS, pad), F32),
            pltpu.VMEM((ROWS, 128), F32),
            pltpu.VMEM((nlat - 1, ROWS, 128), F32),
            pltpu.VMEM((blocks, 5 * ROWS, 128), F32),
            pltpu.VMEM((nlon - 1, blocks, 5 * ROWS, 128), F32),
            dma((2,)),
            dma((nlon - 1,)),
            dma((nlon - 1,)),
            dma((nlon - 1,)),
            dma((nlon - 1,)),
            dma((nlat - 1,)),
            dma((nlat - 1,)),
            dma((nlon - 1,)),
            dma((nlon - 1,)),
        ],
        compiler_params=pltpu.CompilerParams(
            collective_id=0, has_side_effects=True, vmem_limit_bytes=40 << 20
        ),
    )(
        dz,
        speed.reshape(tiers, *flat),
        theta.reshape(tiers, *flat),
        dx.reshape(flat),
        area.reshape(flat),
        flux.reshape(flat),
        depth.reshape(flat),
        region.reshape(flat),
        seam.reshape(1, width),
    )
    out = pl.pallas_call(
        functools.partial(finish, width * nlon),
        name="finish",
        out_shape=(
            jax.ShapeDtypeStruct((OCEAN_REGIONS, blocks, ROWS, THERMAL_BINS), F32),
            jax.ShapeDtypeStruct((OCEAN_REGIONS, tiers, height), F32),
            jax.ShapeDtypeStruct((OCEAN_REGIONS, height), F32),
            jax.ShapeDtypeStruct((OCEAN_REGIONS, height), F32),
        ),
        in_specs=[vmem],
        out_specs=(vmem,) * 4,
        compiler_params=pltpu.CompilerParams(vmem_limit_bytes=8 << 20),
    )(raw)
    classes = out[0].reshape(OCEAN_REGIONS, height, THERMAL_BINS)
    return (classes, jnp.swapaxes(out[1], 1, 2), out[2], out[3])


def solution(mesh):
    in_specs = (
        P(None, "lat", "lon"),
        P(None, "lat", "lon"),
        P(),
        P("lat", "lon"),
        P("lat", "lon"),
        P("lat", "lon"),
        P("lat", "lon"),
        P("lat", "lon"),
        P("lon"),
    )
    out_specs = (P(None, "lat", None), P(None, "lat", None), P(None, "lat"), P(None, "lat"))
    return jax.shard_map(body, mesh=mesh, in_specs=in_specs, out_specs=out_specs, check_vma=False)
```

```python
import functools
import math

import jax
import jax.numpy as jnp
from jax import lax
from jax.experimental import pallas as pl
from jax.experimental.pallas import tpu as pltpu
from jax.sharding import PartitionSpec as P

THERMAL_BINS = 128
OCEAN_REGIONS = 4
THERMAL_FLOOR = -2.0
THERMAL_RANGE = 32.0

ROWS = 8
DIGIT = 16
HIGHS = THERMAL_BINS // DIGIT
PAIRS = OCEAN_REGIONS // 2
GROUP = 4
STRIDE = 32
CUTS = (2, 4, 6)
MESH = pl.DeviceIdType.MESH
NT = (((1,), (1,)), ((), ()))
HIGHEST = lax.Precision.HIGHEST
BF = jnp.bfloat16
F32 = jnp.float32


def iota(shape, dim):
    return lax.broadcasted_iota(jnp.int32, shape, dim)


def two_parts(x):
    high = x.astype(BF).astype(F32)
    return jnp.concatenate([high, x - high], axis=0).astype(BF)


def exact_parts(x):
    high = x.astype(BF).astype(F32)
    rest = x - high
    mid = rest.astype(BF).astype(F32)
    return jnp.concatenate([high.astype(BF), mid.astype(BF), (rest - mid).astype(BF)], axis=0)


def kernel(
    nlon, nlat,
    dz_h, speed_h, theta_h, dx_h, area_h, flux_h, depth_h, region_h, seam_h,
    raw,
    dz, speed, theta, dx_all, area, flux, depth, region, seam,
    edge, edge_in, top, top_in, cap, total, total_in, buf, got,
    big_sem, small_sem, edge_sem, top_send, top_recv, tot_send, tot_recv,
    sum_send, sum_recv,
):
    tiers, blocks, _, width = theta_h.shape
    mylon, mylat = lax.axis_index("lon"), lax.axis_index("lat")
    last = blocks - 1

    barrier = pltpu.get_barrier_semaphore()
    for step in range(1, nlon):
        peer = lax.rem(mylon + step, nlon)
        pl.semaphore_signal(barrier, inc=1, device_id=(peer, mylat), device_id_type=MESH)
    for step in range(1, nlat):
        peer = lax.rem(mylat + step, nlat)
        pl.semaphore_signal(barrier, inc=1, device_id=(mylon, peer), device_id_type=MESH)

    small = [
        pltpu.make_async_copy(src, dst, small_sem.at[n])
        for n, (src, dst) in enumerate(
            [
                (area_h, area),
                (flux_h, flux),
                (region_h, region),
                (depth_h, depth),
                (dx_h, dx_all),
                (dz_h, dz),
                (seam_h, seam),
            ]
        )
    ]

    def theta_copy(b):
        return pltpu.make_async_copy(theta_h.at[:, b], theta.at[b], big_sem.at[0, b])

    def speed_copy(b):
        return pltpu.make_async_copy(speed_h.at[:, b], speed.at[b], big_sem.at[1, b])

    for copy in small:
        copy.start()
    theta_copy(0).start()
    theta_copy(last).start()
    for b in range(blocks):
        speed_copy(b).start()
        if b + 1 < last:
            theta_copy(b + 1).start()
    for copy in small:
        copy.wait()

    def flux_total():
        sums = [jnp.zeros((ROWS, width), F32)] * OCEAN_REGIONS
        for jb in range(blocks):
            product = flux[jb] * area[jb]
            for b in range(OCEAN_REGIONS):
                sums[b] = sums[b] + jnp.where(region[jb] == b, product, 0.0)
        total[...] = jnp.zeros_like(total)
        for b in range(OCEAN_REGIONS):
            line = jnp.sum(sums[b], axis=0, keepdims=True)
            for at in range(0, width, 128):
                piece = line[:, at : at + 128]
                folded = piece if at == 0 else folded + piece
            total[pl.ds(b, 1), :] = folded

    flux_total()
    theta_copy(0).wait()
    theta_copy(last).wait()
    edge[...] = jnp.zeros_like(edge)
    top[...] = jnp.zeros_like(top)
    for k in range(tiers):
        edge[pl.ds(k, 1), :] = theta[0, k, pl.ds(0, 1), :]
        top[pl.ds(k, 1), :] = theta[last, k, pl.ds(ROWS - 1, 1), :]
    edge[pl.ds(tiers, 1), :] = depth[0, pl.ds(0, 1), :].astype(F32)
    top[pl.ds(tiers, 1), :] = depth[last, pl.ds(ROWS - 1, 1), :].astype(F32)

    edge_copy = pltpu.make_async_remote_copy(
        edge, edge_in, edge_sem.at[0], edge_sem.at[1],
        device_id=(mylon, lax.rem(mylat + nlat - 1, nlat)), device_id_type=MESH,
    )

    def to_lon(src, dst, send, recv, step):
        return pltpu.make_async_remote_copy(
            src, dst.at[step - 1], send.at[step - 1], recv.at[step - 1],
            device_id=(lax.rem(mylon + step, nlon), mylat), device_id_type=MESH,
        )

    def to_lat(step):
        return pltpu.make_async_remote_copy(
            total, total_in.at[step - 1], tot_send.at[step - 1], tot_recv.at[step - 1],
            device_id=(mylon, lax.rem(mylat + step, nlat)), device_id_type=MESH,
        )

    def across(offset):
        peer = mylon
        for bit in range(nlon.bit_length() - 1):
            stride = 1 << bit
            if offset & stride:
                peer = peer + stride * (1 - 2 * lax.rem(lax.div(mylon, stride), 2))
        return peer

    def share(offset, src, dst):
        return pltpu.make_async_remote_copy(
            src, dst, sum_send.at[offset - 1], sum_recv.at[offset - 1],
            device_id=(across(offset), mylat), device_id_type=MESH,
        )

    def tree(parts):
        while len(parts) > 1:
            parts = [parts[n] + parts[n + 1] for n in range(0, len(parts), 2)]
        return parts[0]

    def first_sends():
        pl.semaphore_wait(barrier, nlon - 1 + nlat - 1)
        edge_copy.start()
        for step in range(1, nlat):
            to_lat(step).start()

        @pl.when(mylat == nlat - 1)
        def _():
            for step in range(1, nlon):
                to_lon(top, top_in, top_send, top_recv, step).start()

    def compute(jb, cap_row):
        reg = region[jb].astype(F32)
        dx = dx_all[jb]
        deep = depth[jb].astype(F32)

        def above(own, k):
            row = theta[jb + 1, k, pl.ds(0, 1), :] if cap_row is None else cap_row(k)
            return jnp.concatenate([own[1:], row], axis=0)

        def twice(x, y):
            return jnp.concatenate([x, y], axis=0).astype(BF)

        depth_row = (
            depth[jb + 1, pl.ds(0, 1), :].astype(F32) if cap_row is None else cap_row(tiers)
        )
        wet = jnp.minimum(deep, jnp.concatenate([deep[1:], depth_row], axis=0))
        one, zero = jnp.ones((2 * ROWS, width), BF), jnp.zeros((2 * ROWS, width), BF)
        reg2 = twice(reg, reg - 1.0)
        here = [
            jnp.where(reg2 == jnp.asarray(2 * n, BF), one, zero) for n in range(PAIRS)
        ]
        heat = jnp.zeros((ROWS, width), F32)
        warm = jnp.zeros((ROWS, width), F32)
        water = jnp.zeros((ROWS, width), F32)
        kept = []
        accs = [None, None]
        for first in range(0, tiers, GROUP):
            tents, picks = [], []
            side = (first // GROUP) % 2
            for k in range(first, min(first + GROUP, tiers)):
                th = theta[jb, k]
                both = th + above(th, k)
                face = 0.5 * both
                volume = jnp.where(wet > float(k), dz[k] * dx, 0.0)
                moved = volume * speed[jb, k]
                heat = heat + moved * face
                warm = warm + volume * face
                water = water + volume
                place = jnp.clip(
                    (face - THERMAL_FLOOR) * (THERMAL_BINS / THERMAL_RANGE),
                    0.0, THERMAL_BINS - 1.0,
                )
                low = jnp.minimum(jnp.floor(place), THERMAL_BINS - 2.0)
                upper = moved * (place - low)
                under = moved - upper
                high = jnp.floor(low * (1.0 / DIGIT))
                digit = low - DIGIT * high
                high2 = twice(high, high)
                digit2 = twice(digit, digit - 8.0) if side == 0 else twice(digit - 8.0, digit)
                under_h = under.astype(BF).astype(F32)
                upper_h = upper.astype(BF).astype(F32)
                under_l, upper_l = under - under_h, upper - upper_h
                hits = [digit2 == jnp.asarray(n, BF) for n in range(-1, 8)]
                tent = []
                for low_half, high_half in ((under_h, upper_h), (under_l, upper_l)):
                    low2, up2 = twice(low_half, low_half), twice(high_half, high_half)
                    for n in range(8):
                        tent.append(
                            jnp.where(hits[n + 1], low2, jnp.where(hits[n], up2, zero))
                        )
                ending = twice(digit, digit) == jnp.asarray(DIGIT - 1, BF)
                tent.append(jnp.where(ending, twice(upper_h, upper_l), zero))
                tents.append(jnp.concatenate(tent, axis=0))
                kept.append(two_parts(moved))
                chosen = [high2 == jnp.asarray(n, BF) for n in range(HIGHS)]
                picks.append(
                    jnp.concatenate(
                        [
                            jnp.where(chosen[n], here[pair], zero)
                            for pair in range(PAIRS)
                            for n in range(HIGHS)
                        ],
                        axis=0,
                    )
                )
            part = lax.dot_general(
                jnp.concatenate(tents, axis=1), jnp.concatenate(picks, axis=1), NT,
                preferred_element_type=F32,
            )
            accs[side] = part if accs[side] is None else accs[side] + part

        lane = iota((ROWS, 128), 1)
        row = iota((ROWS, 128), 0)

        def align(x, slot):
            source = (lane + row + (128 - slot)) % 128
            return jnp.take_along_axis(x, source, axis=1, mode="promise_in_bounds")

        for pair in range(PAIRS):
            cols = [x[:, 128 * pair : 128 * pair + 128] for x in accs]
            held = []
            for half in range(2):
                out = jnp.zeros((ROWS, 128), F32)
                for n in range(8):
                    ats = (16 * n + 8 * half, 16 * n + 8 * (1 - half))
                    one_tent = tree(
                        [x[p + at : p + at + ROWS] for x, at in zip(cols, ats) for p in (0, 128)]
                    )
                    out = jnp.where(lane % 8 == n, align(one_tent, n), out)
                held.append(out)
            final = tree(
                [align(x[256 : 256 + ROWS] + x[256 + ROWS :], DIGIT) for x in cols]
            )
            held[0] = held[0] + jnp.where(lane % 8 == 0, final, 0.0)
            left = lane % 16 < 8
            buf[jb, pl.ds(2 * pair * ROWS, ROWS), :] = jnp.where(
                left, held[0], pltpu.roll(held[1], 8, 1)
            )
            buf[jb, pl.ds((2 * pair + 1) * ROWS, ROWS), :] = jnp.where(
                left, pltpu.roll(held[0], 120, 1), held[1]
            )
        kept = kept + [two_parts(heat), two_parts(warm), two_parts(water)]
        kept.append(two_parts(flux[jb] * area[jb]))
        nothing = jnp.zeros((ROWS, width), F32)
        basin = []
        for b in range(OCEAN_REGIONS):
            basin += [twice(jnp.where(reg == float(b), 1.0, 0.0), nothing), zero]
        table = lax.dot_general(
            jnp.concatenate(kept, axis=0), jnp.concatenate(basin, axis=0), NT,
            preferred_element_type=F32,
        )
        line = jnp.zeros((ROWS, 128), F32)
        for k in range(len(kept)):
            at = 2 * ROWS * k
            whole = table[at : at + ROWS] + table[at + ROWS : at + 2 * ROWS]
            line = jnp.where(lane % STRIDE == k, align(whole, k), line)
        buf[jb, pl.ds(OCEAN_REGIONS * ROWS, ROWS), :] = line

    def publish(jb):
        for offset in range(1, nlon):
            share(offset, buf.at[jb], got.at[offset - 1, jb]).start()

    def northern_row():
        edge_copy.wait()

        @pl.when(mylat < nlat - 1)
        def _():
            cap[...] = edge_in[...]

        @pl.when(mylat == nlat - 1)
        def _():
            found = jnp.zeros((3 * top.shape[0], width), F32)
            for step in range(nlon):
                if step:
                    to_lon(top, top_in, top_send, top_recv, step).wait()
                block = top_in[step - 1] if step else top[...]
                owner = lax.rem(mylon + nlon - step, nlon)
                here = iota((width, width), 0) + owner * width == seam[...]
                found = found + jnp.dot(
                    exact_parts(block), jnp.where(here, 1.0, 0.0).astype(BF),
                    preferred_element_type=F32,
                )
            n = top.shape[0]
            cap[...] = found[:n] + found[n : 2 * n] + found[2 * n :]

    def southern_flux():
        for step in range(1, nlat):
            to_lat(step).wait()
        before = jnp.zeros(total.shape, F32)
        for step in range(1, nlat):
            before = before + jnp.where(mylat >= step, total_in[step - 1], 0.0)
        lane = iota((ROWS, 128), 1)
        line = jnp.zeros((1, 128), F32)
        for b in range(OCEAN_REGIONS):
            line = jnp.where(
                lane[:1] == b * STRIDE + tiers + 4,
                jnp.sum(before[b : b + 1], axis=1, keepdims=True), line,
            )
        at = OCEAN_REGIONS * ROWS
        buf[last, pl.ds(at, 1), :] = buf[last, pl.ds(at, 1), :] + line

    cuts = [0] + [at for at in CUTS if at < blocks] + [blocks]
    for segment in range(len(cuts) - 1):
        members = range(cuts[segment], cuts[segment + 1])
        final = members[-1] == last
        for jb in members:
            speed_copy(jb).wait()
            if 0 < jb + 1 < last:
                theta_copy(jb + 1).wait()
        if final:
            northern_row()
        for jb in members:
            compute(jb, (lambda k: cap[pl.ds(k, 1), :]) if jb == last else None)
        if segment == 0:
            first_sends()
        if final:
            southern_flux()
        for jb in members:
            publish(jb)
    for offset in range(1, nlon):
        share(offset, buf, got.at[offset - 1]).wait()
    for jb in range(blocks):
        both = tree([buf[jb]] + [got[offset - 1, jb] for offset in range(1, nlon)])
        raw[jb] = both.reshape(OCEAN_REGIONS + 1, ROWS, 128)


def finish(width_total, height_total, raw, class_o, stream_o, heat_o, implied_o):
    blocks, height = raw.shape[0], stream_o.shape[2]
    tiers = stream_o.shape[1]
    unit_scale = math.sqrt(THERMAL_BINS / (width_total * tiers))
    for b in range(OCEAN_REGIONS):
        class_o[b] = unit_scale * raw[:blocks, b]
    table = raw[:blocks, OCEAN_REGIONS].reshape(height, 128)
    dst, src = iota((128, 128), 0), iota((128, 128), 1)
    chain = (src // STRIDE == dst // STRIDE) & (src <= dst) & (src % STRIDE < tiers)
    stream = unit_scale * lax.dot_general(
        chain.astype(F32), table, NT, precision=HIGHEST, preferred_element_type=F32
    )
    for b in range(OCEAN_REGIONS):
        stream_o[b] = stream[b * STRIDE : b * STRIDE + tiers]
    row, lane = iota((6 * ROWS, 128), 0), iota((6 * ROWS, 128), 1)
    kind, place, slot = row // ROWS, row % ROWS, lane % STRIDE
    own = place == lane // STRIDE
    choose = (
        ((kind == 0) & own & (slot == tiers))
        | ((kind == 1) & own & (slot < tiers))
        | ((kind == 2) & (slot == tiers + 1))
        | ((kind == 3) & (slot == tiers + 2))
        | ((kind == 4) & own & (slot == tiers + 3))
        | ((kind == 5) & own & (slot == tiers + 4))
    )
    rows = lax.dot_general(
        choose.astype(F32), table, NT, precision=HIGHEST, preferred_element_type=F32
    )
    mean = rows[2 * ROWS : 3 * ROWS] / rows[3 * ROWS : 4 * ROWS]
    heat = (unit_scale / 16.0) * (rows[:ROWS] - rows[ROWS : 2 * ROWS] * mean)
    heat_o[...] = heat[:OCEAN_REGIONS]
    until = (iota((height, height), 0) <= iota((height, height), 1)).astype(F32)
    run = jnp.dot(
        rows[4 * ROWS : 5 * ROWS], until, precision=HIGHEST, preferred_element_type=F32
    )
    before = jnp.sum(rows[5 * ROWS :], axis=1, keepdims=True)
    implied = (2.0 / math.sqrt(width_total * height_total)) * (before + run)
    implied_o[...] = implied[:OCEAN_REGIONS]


def body(speed, theta, dz, dx, area, flux, depth, region, seam):
    tiers, height, width = theta.shape
    nlon, nlat = lax.axis_size("lon"), lax.axis_size("lat")
    blocks = height // ROWS
    edge_rows = -(-(tiers + 1) // 8) * 8
    flat = (blocks, ROWS, width)
    any_spec = pl.BlockSpec(memory_space=pltpu.HBM)
    vmem = pl.BlockSpec(memory_space=pltpu.VMEM)
    dma = pltpu.SemaphoreType.DMA
    raw = pl.pallas_call(
        functools.partial(kernel, nlon, nlat),
        name="transport",
        out_shape=pltpu.VMEM((blocks, OCEAN_REGIONS + 1, ROWS, 128), F32),
        in_specs=[any_spec] * 9,
        out_specs=vmem,
        scratch_shapes=[
            pltpu.SMEM((tiers,), F32),
            pltpu.VMEM((blocks, tiers, ROWS, width), F32),
            pltpu.VMEM((blocks, tiers, ROWS, width), F32),
            pltpu.VMEM(flat, F32),
            pltpu.VMEM(flat, F32),
            pltpu.VMEM(flat, F32),
            pltpu.VMEM(flat, jnp.int32),
            pltpu.VMEM(flat, jnp.int32),
            pltpu.VMEM((1, width), jnp.int32),
            pltpu.VMEM((edge_rows, width), F32),
            pltpu.VMEM((edge_rows, width), F32),
            pltpu.VMEM((edge_rows, width), F32),
            pltpu.VMEM((nlon - 1, edge_rows, width), F32),
            pltpu.VMEM((edge_rows, width), F32),
            pltpu.VMEM((ROWS, 128), F32),
            pltpu.VMEM((nlat - 1, ROWS, 128), F32),
            pltpu.VMEM((blocks, 5 * ROWS, 128), F32),
            pltpu.VMEM((nlon - 1, blocks, 5 * ROWS, 128), F32),
            dma((2, blocks)),
            dma((7,)),
            dma((2,)),
            dma((nlon - 1,)),
            dma((nlon - 1,)),
            dma((nlat - 1,)),
            dma((nlat - 1,)),
            dma((nlon - 1,)),
            dma((nlon - 1,)),
        ],
        compiler_params=pltpu.CompilerParams(
            collective_id=0, has_side_effects=True, vmem_limit_bytes=40 << 20
        ),
    )(
        *[
            pltpu.with_memory_space_constraint(x, pltpu.HBM)
            for x in (
                dz,
                speed.reshape(tiers, *flat),
                theta.reshape(tiers, *flat),
                dx.reshape(flat),
                area.reshape(flat),
                flux.reshape(flat),
                depth.reshape(flat),
                region.reshape(flat),
                seam.reshape(1, width),
            )
        ]
    )
    out = pl.pallas_call(
        functools.partial(finish, width * nlon, height * nlat),
        name="finish",
        out_shape=(
            jax.ShapeDtypeStruct((OCEAN_REGIONS, blocks, ROWS, THERMAL_BINS), F32),
            jax.ShapeDtypeStruct((OCEAN_REGIONS, tiers, height), F32),
            jax.ShapeDtypeStruct((OCEAN_REGIONS, height), F32),
            jax.ShapeDtypeStruct((OCEAN_REGIONS, height), F32),
        ),
        in_specs=[vmem],
        out_specs=(vmem,) * 4,
        compiler_params=pltpu.CompilerParams(vmem_limit_bytes=8 << 20),
    )(raw)
    classes = out[0].reshape(OCEAN_REGIONS, height, THERMAL_BINS)
    return (classes, jnp.swapaxes(out[1], 1, 2), out[2], out[3])


def solution(mesh):
    in_specs = (
        P(None, "lat", "lon"),
        P(None, "lat", "lon"),
        P(),
        P("lat", "lon"),
        P("lat", "lon"),
        P("lat", "lon"),
        P("lat", "lon"),
        P("lat", "lon"),
        P("lon"),
    )
    out_specs = (P(None, "lat", None), P(None, "lat", None), P(None, "lat"), P(None, "lat"))
    return jax.shard_map(body, mesh=mesh, in_specs=in_specs, out_specs=out_specs, check_vma=False)
```

```python
import functools
import math

import jax
import jax.numpy as jnp
from jax import lax
from jax.experimental import pallas as pl
from jax.experimental.pallas import tpu as pltpu
from jax.sharding import PartitionSpec as P

THERMAL_BINS = 128
OCEAN_REGIONS = 4
THERMAL_FLOOR = -2.0
THERMAL_RANGE = 32.0

ROWS = 8
DIGIT = 16
HIGHS = THERMAL_BINS // DIGIT
PAIRS = OCEAN_REGIONS // 2
GROUP = 4
STRIDE = 32
EARLY = 2
LATE = 1
MESH = pl.DeviceIdType.MESH
NT = (((1,), (1,)), ((), ()))
HIGHEST = lax.Precision.HIGHEST
BF = jnp.bfloat16
F32 = jnp.float32


def iota(shape, dim):
    return lax.broadcasted_iota(jnp.int32, shape, dim)


def two_parts(x):
    high = x.astype(BF).astype(F32)
    return jnp.concatenate([high, x - high], axis=0).astype(BF)


def exact_parts(x):
    high = x.astype(BF).astype(F32)
    rest = x - high
    mid = rest.astype(BF).astype(F32)
    return jnp.concatenate([high.astype(BF), mid.astype(BF), (rest - mid).astype(BF)], axis=0)


def kernel(
    nlon, nlat,
    dz_h, speed_h, theta_h, dx_h, area_h, flux_h, depth_h, region_h, seam_h,
    raw,
    dz, speed, theta, dx_all, area, flux, depth, region, seam,
    edge, edge_in, top, top_in, cap, total, total_in, buf, got,
    big_sem, small_sem, edge_sem, top_send, top_recv, tot_send, tot_recv,
    sum_send, sum_recv,
):
    tiers, blocks, _, width = theta_h.shape
    mylon, mylat = lax.axis_index("lon"), lax.axis_index("lat")
    last = blocks - 1

    barrier = pltpu.get_barrier_semaphore()
    for step in range(1, nlon):
        peer = lax.rem(mylon + step, nlon)
        pl.semaphore_signal(barrier, inc=1, device_id=(peer, mylat), device_id_type=MESH)
    for step in range(1, nlat):
        peer = lax.rem(mylat + step, nlat)
        pl.semaphore_signal(barrier, inc=1, device_id=(mylon, peer), device_id_type=MESH)

    small = [
        pltpu.make_async_copy(src, dst, small_sem.at[n])
        for n, (src, dst) in enumerate(
            [
                (area_h, area),
                (flux_h, flux),
                (region_h, region),
                (depth_h, depth),
                (dx_h, dx_all),
                (dz_h, dz),
                (seam_h, seam),
            ]
        )
    ]

    def theta_copy(b):
        return pltpu.make_async_copy(theta_h.at[:, b], theta.at[b], big_sem.at[0, b])

    def speed_copy(b):
        return pltpu.make_async_copy(speed_h.at[:, b], speed.at[b], big_sem.at[1, b])

    for copy in small:
        copy.start()
    theta_copy(0).start()
    theta_copy(last).start()
    for b in range(blocks):
        speed_copy(b).start()
        if b + 1 < last:
            theta_copy(b + 1).start()
    for copy in small:
        copy.wait()

    def flux_total():
        sums = [jnp.zeros((ROWS, width), F32)] * OCEAN_REGIONS
        for jb in range(blocks):
            product = flux[jb] * area[jb]
            for b in range(OCEAN_REGIONS):
                sums[b] = sums[b] + jnp.where(region[jb] == b, product, 0.0)
        lane = iota((1, 128), 1)
        line = jnp.zeros((1, 128), F32)
        for b in range(OCEAN_REGIONS):
            line = jnp.where(
                lane == b * STRIDE + tiers + 4,
                jnp.sum(jnp.sum(sums[b], axis=0, keepdims=True), axis=1, keepdims=True),
                line,
            )
        total[...] = line

    flux_total()
    theta_copy(0).wait()
    theta_copy(last).wait()
    edge[...] = jnp.zeros_like(edge)
    top[...] = jnp.zeros_like(top)
    for k in range(tiers):
        edge[pl.ds(k, 1), :] = theta[0, k, pl.ds(0, 1), :]
        top[pl.ds(k, 1), :] = theta[last, k, pl.ds(ROWS - 1, 1), :]
    edge[pl.ds(tiers, 1), :] = depth[0, pl.ds(0, 1), :].astype(F32)
    top[pl.ds(tiers, 1), :] = depth[last, pl.ds(ROWS - 1, 1), :].astype(F32)

    edge_copy = pltpu.make_async_remote_copy(
        edge, edge_in, edge_sem.at[0], edge_sem.at[1],
        device_id=(mylon, lax.rem(mylat + nlat - 1, nlat)), device_id_type=MESH,
    )

    def to_lon(src, dst, send, recv, step):
        return pltpu.make_async_remote_copy(
            src, dst.at[step - 1], send.at[step - 1], recv.at[step - 1],
            device_id=(lax.rem(mylon + step, nlon), mylat), device_id_type=MESH,
        )

    def to_lat(step):
        return pltpu.make_async_remote_copy(
            total, total_in.at[step - 1], tot_send.at[step - 1], tot_recv.at[step - 1],
            device_id=(mylon, lax.rem(mylat + step, nlat)), device_id_type=MESH,
        )

    def across(offset):
        peer = mylon
        for bit in range(nlon.bit_length() - 1):
            stride = 1 << bit
            if offset & stride:
                peer = peer + stride * (1 - 2 * lax.rem(lax.div(mylon, stride), 2))
        return peer

    def share(offset, src, dst):
        return pltpu.make_async_remote_copy(
            src, dst, sum_send.at[offset - 1], sum_recv.at[offset - 1],
            device_id=(across(offset), mylat), device_id_type=MESH,
        )

    def tree(parts):
        while len(parts) > 1:
            parts = [parts[n] + parts[n + 1] for n in range(0, len(parts), 2)]
        return parts[0]

    def first_sends():
        pl.semaphore_wait(barrier, nlon - 1 + nlat - 1)
        for step in range(1, nlat):
            to_lat(step).start()
        edge_copy.start()

        @pl.when(mylat == nlat - 1)
        def _():
            for step in range(1, nlon):
                to_lon(top, top_in, top_send, top_recv, step).start()

    def main(jb, cap_row):
        reg = region[jb].astype(F32)
        dx = dx_all[jb]
        deep = depth[jb].astype(F32)

        def above(own, k):
            row = theta[jb + 1, k, pl.ds(0, 1), :] if cap_row is None else cap_row(k)
            return jnp.concatenate([own[1:], row], axis=0)

        def twice(x, y):
            return jnp.concatenate([x, y], axis=0).astype(BF)

        depth_row = (
            depth[jb + 1, pl.ds(0, 1), :].astype(F32) if cap_row is None else cap_row(tiers)
        )
        wet = jnp.minimum(deep, jnp.concatenate([deep[1:], depth_row], axis=0))
        one, zero = jnp.ones((2 * ROWS, width), BF), jnp.zeros((2 * ROWS, width), BF)
        reg2 = twice(reg, reg - 1.0)
        here = [
            jnp.where(reg2 == jnp.asarray(2 * n, BF), one, zero) for n in range(PAIRS)
        ]
        heat = jnp.zeros((ROWS, width), F32)
        warm = jnp.zeros((ROWS, width), F32)
        water = jnp.zeros((ROWS, width), F32)
        kept = []
        accs = [None, None]
        for first in range(0, tiers, GROUP):
            tents, picks = [], []
            side = (first // GROUP) % 2
            for k in range(first, min(first + GROUP, tiers)):
                th = theta[jb, k]
                both = th + above(th, k)
                face = 0.5 * both
                volume = jnp.where(wet > float(k), dz[k] * dx, 0.0)
                moved = volume * speed[jb, k]
                heat = heat + moved * face
                warm = warm + volume * face
                water = water + volume
                place = jnp.clip(
                    (face - THERMAL_FLOOR) * (THERMAL_BINS / THERMAL_RANGE),
                    0.0, THERMAL_BINS - 1.0,
                )
                low = jnp.minimum(jnp.floor(place), THERMAL_BINS - 2.0)
                upper = moved * (place - low)
                under = moved - upper
                high = jnp.floor(low * (1.0 / DIGIT))
                digit = low - DIGIT * high
                high2 = twice(high, high)
                digit2 = twice(digit, digit - 8.0) if side == 0 else twice(digit - 8.0, digit)
                under_h = under.astype(BF).astype(F32)
                upper_h = upper.astype(BF).astype(F32)
                under_l, upper_l = under - under_h, upper - upper_h
                hits = [digit2 == jnp.asarray(n, BF) for n in range(-1, 8)]
                tent = []
                for low_half, high_half in ((under_h, upper_h), (under_l, upper_l)):
                    low2, up2 = twice(low_half, low_half), twice(high_half, high_half)
                    for n in range(8):
                        tent.append(
                            jnp.where(hits[n + 1], low2, jnp.where(hits[n], up2, zero))
                        )
                ending = twice(digit, digit) == jnp.asarray(DIGIT - 1, BF)
                tent.append(jnp.where(ending, twice(upper_h, upper_l), zero))
                tents.append(jnp.concatenate(tent, axis=0))
                kept.append(two_parts(moved))
                chosen = [high2 == jnp.asarray(n, BF) for n in range(HIGHS)]
                picks.append(
                    jnp.concatenate(
                        [
                            jnp.where(chosen[n], here[pair], zero)
                            for pair in range(PAIRS)
                            for n in range(HIGHS)
                        ],
                        axis=0,
                    )
                )
            part = lax.dot_general(
                jnp.concatenate(tents, axis=1), jnp.concatenate(picks, axis=1), NT,
                preferred_element_type=F32,
            )
            accs[side] = part if accs[side] is None else accs[side] + part

        kept = kept + [two_parts(heat), two_parts(warm), two_parts(water)]
        kept.append(two_parts(flux[jb] * area[jb]))
        nothing = jnp.zeros((ROWS, width), F32)
        basin = []
        for b in range(OCEAN_REGIONS):
            basin += [twice(jnp.where(reg == float(b), 1.0, 0.0), nothing), zero]
        table = lax.dot_general(
            jnp.concatenate(kept, axis=0), jnp.concatenate(basin, axis=0), NT,
            preferred_element_type=F32,
        )
        return accs, table

    def tail(jb, accs, table):
        lane = iota((ROWS, 128), 1)
        row = iota((ROWS, 128), 0)

        def align(x, slot):
            source = (lane + row + (128 - slot)) % 128
            return jnp.take_along_axis(x, source, axis=1, mode="promise_in_bounds")

        for pair in range(PAIRS):
            cols = [x[:, 128 * pair : 128 * pair + 128] for x in accs]
            held = []
            for half in range(2):
                out = jnp.zeros((ROWS, 128), F32)
                for n in range(8):
                    ats = (16 * n + 8 * half, 16 * n + 8 * (1 - half))
                    one_tent = tree(
                        [x[p + at : p + at + ROWS] for x, at in zip(cols, ats) for p in (0, 128)]
                    )
                    out = jnp.where(lane % 8 == n, align(one_tent, n), out)
                held.append(out)
            final = tree(
                [align(x[256 : 256 + ROWS] + x[256 + ROWS :], DIGIT) for x in cols]
            )
            held[0] = held[0] + jnp.where(lane % 8 == 0, final, 0.0)
            left = lane % 16 < 8
            buf[jb, pl.ds(2 * pair * ROWS, ROWS), :] = jnp.where(
                left, held[0], pltpu.roll(held[1], 8, 1)
            )
            buf[jb, pl.ds((2 * pair + 1) * ROWS, ROWS), :] = jnp.where(
                left, pltpu.roll(held[0], 120, 1), held[1]
            )
        line = jnp.zeros((ROWS, 128), F32)
        for k in range(table.shape[0] // (2 * ROWS)):
            at = 2 * ROWS * k
            whole = table[at : at + ROWS] + table[at + ROWS : at + 2 * ROWS]
            line = jnp.where(lane % STRIDE == k, align(whole, k), line)
        buf[jb, pl.ds(OCEAN_REGIONS * ROWS, ROWS), :] = line

    def publish(jb):
        for offset in range(nlon - 1, 0, -1):
            share(offset, buf.at[jb], got.at[offset - 1, jb]).start()

    def await_north():
        edge_copy.wait()

        @pl.when(mylat == nlat - 1)
        def _():
            for step in range(1, nlon):
                to_lon(top, top_in, top_send, top_recv, step).wait()

    def northern_row():
        n = top.shape[0]
        folded = []
        for step in range(nlon):
            block = top_in[step - 1] if step else top[...]
            owner = lax.rem(mylon + nlon - step, nlon)
            here = iota((width, width), 0) == seam[...] - owner * width
            folded.append(
                jnp.dot(
                    exact_parts(block), jnp.where(here, 1.0, 0.0).astype(BF),
                    preferred_element_type=F32,
                )
            )
        found = sum(folded[1:], folded[0])
        row = found[:n] + found[n : 2 * n] + found[2 * n :]
        return jnp.where(mylat == nlat - 1, row, edge_in[...])

    def southern_flux():
        for step in range(1, nlat):
            to_lat(step).wait()
        line = jnp.zeros(total.shape, F32)
        for step in range(1, nlat):
            line = line + jnp.where(mylat >= step, total_in[step - 1], 0.0)
        at = OCEAN_REGIONS * ROWS
        buf[last, pl.ds(at, 1), :] = buf[last, pl.ds(at, 1), :] + line

    def loaded(members):
        for jb in members:
            speed_copy(jb).wait()
            if 0 < jb + 1 < last:
                theta_copy(jb + 1).wait()

    def capped(jb):
        return (lambda k: cap[pl.ds(k, 1), :]) if jb == last else None

    early, late = min(EARLY, last), max(blocks - LATE, min(EARLY, last))
    loaded(range(early))
    pending = []
    for jb in range(early):
        pending.append((jb, main(jb, None)))
    for jb, made in pending:
        tail(jb, *made)
    loaded(range(early, blocks))
    first_sends()
    for jb in range(early):
        publish(jb)
    ahead = None
    for jb in range(early, late):
        made = main(jb, None)
        if ahead is not None:
            tail(*ahead)
            publish(ahead[0])
        ahead = (jb, *made)
    if ahead is not None:
        tail(*ahead)
    await_north()
    if ahead is not None:
        publish(ahead[0])
    cap[...] = northern_row()
    ahead = None
    for jb in range(late, blocks):
        made = main(jb, capped(jb))
        if ahead is not None:
            tail(*ahead)
            publish(ahead[0])
        ahead = (jb, *made)
    tail(*ahead)
    southern_flux()
    publish(last)
    for offset in range(1, nlon):
        share(offset, buf, got.at[offset - 1]).wait()
    for jb in range(blocks):
        both = tree([buf[jb]] + [got[offset - 1, jb] for offset in range(1, nlon)])
        raw[jb] = both.reshape(OCEAN_REGIONS + 1, ROWS, 128)


def finish(width_total, height_total, raw, class_o, stream_o, heat_o, implied_o):
    blocks, height = raw.shape[0], stream_o.shape[2]
    tiers = stream_o.shape[1]
    unit_scale = math.sqrt(THERMAL_BINS / (width_total * tiers))
    for b in range(OCEAN_REGIONS):
        class_o[b] = unit_scale * raw[:blocks, b]
    table = raw[:blocks, OCEAN_REGIONS].reshape(height, 128)
    dst, src = iota((128, 128), 0), iota((128, 128), 1)
    chain = (src // STRIDE == dst // STRIDE) & (src <= dst) & (src % STRIDE < tiers)
    stream = unit_scale * lax.dot_general(
        chain.astype(F32), table, NT, precision=HIGHEST, preferred_element_type=F32
    )
    for b in range(OCEAN_REGIONS):
        stream_o[b] = stream[b * STRIDE : b * STRIDE + tiers]
    row, lane = iota((6 * ROWS, 128), 0), iota((6 * ROWS, 128), 1)
    kind, place, slot = row // ROWS, row % ROWS, lane % STRIDE
    own = place == lane // STRIDE
    choose = (
        ((kind == 0) & own & (slot == tiers))
        | ((kind == 1) & own & (slot < tiers))
        | ((kind == 2) & (slot == tiers + 1))
        | ((kind == 3) & (slot == tiers + 2))
        | ((kind == 4) & own & (slot == tiers + 3))
        | ((kind == 5) & own & (slot == tiers + 4))
    )
    rows = lax.dot_general(
        choose.astype(F32), table, NT, precision=HIGHEST, preferred_element_type=F32
    )
    mean = rows[2 * ROWS : 3 * ROWS] / rows[3 * ROWS : 4 * ROWS]
    heat = (unit_scale / 16.0) * (rows[:ROWS] - rows[ROWS : 2 * ROWS] * mean)
    heat_o[...] = heat[:OCEAN_REGIONS]
    until = (iota((height, height), 0) <= iota((height, height), 1)).astype(F32)
    run = jnp.dot(
        rows[4 * ROWS : 5 * ROWS], until, precision=HIGHEST, preferred_element_type=F32
    )
    before = jnp.sum(rows[5 * ROWS :], axis=1, keepdims=True)
    implied = (2.0 / math.sqrt(width_total * height_total)) * (before + run)
    implied_o[...] = implied[:OCEAN_REGIONS]


def body(speed, theta, dz, dx, area, flux, depth, region, seam):
    tiers, height, width = theta.shape
    nlon, nlat = lax.axis_size("lon"), lax.axis_size("lat")
    blocks = height // ROWS
    edge_rows = -(-(tiers + 1) // 8) * 8
    flat = (blocks, ROWS, width)
    any_spec = pl.BlockSpec(memory_space=pltpu.HBM)
    vmem = pl.BlockSpec(memory_space=pltpu.VMEM)
    dma = pltpu.SemaphoreType.DMA
    raw = pl.pallas_call(
        functools.partial(kernel, nlon, nlat),
        name="transport",
        out_shape=pltpu.VMEM((blocks, OCEAN_REGIONS + 1, ROWS, 128), F32),
        in_specs=[any_spec] * 9,
        out_specs=vmem,
        scratch_shapes=[
            pltpu.SMEM((tiers,), F32),
            pltpu.VMEM((blocks, tiers, ROWS, width), F32),
            pltpu.VMEM((blocks, tiers, ROWS, width), F32),
            pltpu.VMEM(flat, F32),
            pltpu.VMEM(flat, F32),
            pltpu.VMEM(flat, F32),
            pltpu.VMEM(flat, jnp.int32),
            pltpu.VMEM(flat, jnp.int32),
            pltpu.VMEM((1, width), jnp.int32),
            pltpu.VMEM((edge_rows, width), F32),
            pltpu.VMEM((edge_rows, width), F32),
            pltpu.VMEM((edge_rows, width), F32),
            pltpu.VMEM((nlon - 1, edge_rows, width), F32),
            pltpu.VMEM((edge_rows, width), F32),
            pltpu.VMEM((1, 128), F32),
            pltpu.VMEM((nlat - 1, 1, 128), F32),
            pltpu.VMEM((blocks, 5 * ROWS, 128), F32),
            pltpu.VMEM((nlon - 1, blocks, 5 * ROWS, 128), F32),
            dma((2, blocks)),
            dma((7,)),
            dma((2,)),
            dma((nlon - 1,)),
            dma((nlon - 1,)),
            dma((nlat - 1,)),
            dma((nlat - 1,)),
            dma((nlon - 1,)),
            dma((nlon - 1,)),
        ],
        compiler_params=pltpu.CompilerParams(
            collective_id=0, has_side_effects=True, vmem_limit_bytes=40 << 20
        ),
    )(
        *[
            pltpu.with_memory_space_constraint(x, pltpu.HBM)
            for x in (
                dz,
                speed.reshape(tiers, *flat),
                theta.reshape(tiers, *flat),
                dx.reshape(flat),
                area.reshape(flat),
                flux.reshape(flat),
                depth.reshape(flat),
                region.reshape(flat),
                seam.reshape(1, width),
            )
        ]
    )
    out = pl.pallas_call(
        functools.partial(finish, width * nlon, height * nlat),
        name="finish",
        out_shape=(
            jax.ShapeDtypeStruct((OCEAN_REGIONS, blocks, ROWS, THERMAL_BINS), F32),
            jax.ShapeDtypeStruct((OCEAN_REGIONS, tiers, height), F32),
            jax.ShapeDtypeStruct((OCEAN_REGIONS, height), F32),
            jax.ShapeDtypeStruct((OCEAN_REGIONS, height), F32),
        ),
        in_specs=[vmem],
        out_specs=(vmem,) * 4,
        compiler_params=pltpu.CompilerParams(vmem_limit_bytes=8 << 20),
    )(raw)
    classes = out[0].reshape(OCEAN_REGIONS, height, THERMAL_BINS)
    return (classes, jnp.swapaxes(out[1], 1, 2), out[2], out[3])


def solution(mesh):
    in_specs = (
        P(None, "lat", "lon"),
        P(None, "lat", "lon"),
        P(),
        P("lat", "lon"),
        P("lat", "lon"),
        P("lat", "lon"),
        P("lat", "lon"),
        P("lat", "lon"),
        P("lon"),
    )
    out_specs = (P(None, "lat", None), P(None, "lat", None), P(None, "lat"), P(None, "lat"))
    return jax.shard_map(body, mesh=mesh, in_specs=in_specs, out_specs=out_specs, check_vma=False)
```
